32 devices in a mesh: sky: 8 (over z, y), band: 4 (over x, core).
Axes of the slice: x: 2, y: 2, z: 4, core: 2. Of those that a mesh axis runs over, the one named last changes fastest.
Arguments:
- magnitudes: float32 [4, 8, 16384], P('band', None, 'sky'), may hold values from -7 to 7
- weights: float32 [4, 8, 16384], P('band', None, 'sky'), may hold values from 0.25 to 4
- slots: int32 [4, 8, 16384], P('band', None, 'sky'), may hold values from 0 to 31, as said below
- block_fields: int32 [64, 32], P('sky'), may hold values from 0 to 4096, as said below
- owner: int32 [4096], replicated, may hold values from 0 to 7, as said below
- colors: int32 [4096], replicated, may hold values from 0 to 7
- color_terms: float32 [4, 4], replicated, may hold values from -0.25 to 0.25
Outputs:
- zero_points: float32 [4, 4096], P('band', 'sky')
- star_mags: float32 [4, 16384], P('band', 'sky')
- misfit: float32 [4, 4], P(None, 'band')
The draws below stay inside these ranges and needn't reach their ends.
Inputs may be any that keep to these rules, and one draw needn't show every extreme that they name: `block_fields`: the live entries of each list come first, are distinct, and name fields owned by the block's own sky tile or by the tiles one index below or above it, cyclically over 8 tiles; the remaining entries equal 4096. A list holds 16 or more live entries, and every tile has a block with all 32 live. `owner`: each sky tile owns exactly 512 fields. `slots`: each observation names a live entry of its block's list.
All inputs are finite; a program needn't handle non-finite values.
Results may differ from the reference program's by a relative error of at most 0.00023.
Values sent between devices are 32-bit elements; how exact they have to be, the bound alone decides.
A program may use at most 64 MiB of HBM per device.

```python
import math
import jax
import jax.numpy as jnp
from jax import lax

F = 4096
COLORS = 8
SWEEPS = 4
OBS = 8
LIST = 32
ROWS = 256
BLK_DEV = 8
NBANDS = 4
TILES = 8
F_OWN = 512
NBLOCKS = 64
NSTARS = 16384


def layout(key):
    permuted = jax.random.permutation(jax.random.fold_in(key, 1), F)
    owner = (permuted // F_OWN).astype(jnp.int32)
    inverse = jnp.argsort(permuted, stable=True)
    tile_of = jnp.arange(NBLOCKS) // BLK_DEV
    offsets = jnp.arange(3 * F_OWN)
    nearby = (tile_of[:, None] + offsets[None, :] // F_OWN - 1) % TILES * F_OWN + offsets[None, :] % F_OWN
    candidates = inverse[nearby]
    pick_keys = jax.random.split(jax.random.fold_in(key, 2), NBLOCKS)
    shuffles = jax.vmap(lambda block_key: jax.random.permutation(block_key, 3 * F_OWN))(pick_keys)[:, :LIST]
    picked = jnp.take_along_axis(candidates, shuffles, axis=1)
    live_count = jax.random.randint(jax.random.fold_in(key, 3), (NBLOCKS,), LIST // 2, LIST + 1)
    full_block = tile_of * BLK_DEV + tile_of * 5 % BLK_DEV
    live_count = live_count.at[full_block].set(LIST)
    lists = jnp.where(jnp.arange(LIST)[None, :] < live_count[:, None], picked, F).astype(jnp.int32)
    raw_bits = jax.random.randint(jax.random.fold_in(key, 4), (NBANDS, OBS, NSTARS), 0, 1 << 20)
    star_live = jnp.repeat(live_count, ROWS)
    slot_values = (raw_bits % star_live[None, None, :]).astype(jnp.int32)
    return (owner, lists, slot_values)


def draw_block_fields(key, part):
    return layout(key)[1]


def draw_owner(key, part):
    return layout(key)[0]


def draw_slots(key, part):
    return layout(key)[2]


def draw_magnitudes(key, part):
    owner, lists, slot_values = layout(key)
    expanded = jnp.broadcast_to(lists[None, None, :, :], (NBANDS, OBS, NBLOCKS, LIST))
    field_ids = jnp.take_along_axis(expanded, slot_values.reshape(NBANDS, OBS, NBLOCKS, ROWS), axis=3).reshape(NBANDS, OBS, NSTARS)
    star_tint = jax.random.uniform(jax.random.fold_in(key, 11), (NSTARS,), jnp.float32, -1.0, 1.0)
    band_slope = jax.random.uniform(jax.random.fold_in(key, 12), (NBANDS,), jnp.float32, -1.0, 1.0)
    base_mag = jax.random.uniform(jax.random.fold_in(key, 13), (NSTARS,), jnp.float32, -3.0, 3.0)
    field_off = jax.random.uniform(jax.random.fold_in(key, 14), (NBANDS, F), jnp.float32, -1.0, 1.0)
    noise_term = 0.05 * jnp.clip(jax.random.normal(jax.random.fold_in(key, 15), (NBANDS, OBS, NSTARS), jnp.float32), -2.0, 2.0)
    star_part = base_mag[None, :] + band_slope[:, None] * star_tint[None, :]
    field_part = jax.vmap(jnp.take)(field_off, field_ids)
    return (star_part[:, None, :] + field_part + noise_term).astype(jnp.float32)


def place_ends(result, own_key, least, largest):
    place = [jax.random.randint(jax.random.fold_in(own_key, axis), (), 0, length) for axis, length in enumerate(result.shape)]
    widest = result.shape.index(max(result.shape))
    next_to = place[:widest] + [(place[widest] + 1) % result.shape[widest]] + place[widest + 1:]
    return result.at[tuple(place)].set(least).at[tuple(next_to)].set(largest)


def block_scale(stream_key, extent, cuts, smallest, largest):
    gain, own = 1.0, jax.random.fold_in(stream_key, 6)
    for position, blocks in cuts:
        draws = jnp.exp(jax.random.uniform(jax.random.fold_in(own, position), (blocks,), jnp.float32, smallest / len(cuts), largest / len(cuts)))
        gain = gain * jnp.repeat(draws, extent[position] // blocks).reshape([-1 if axis == position else 1 for axis in range(len(extent))])
    return gain


def setup_inputs(seed: int = 0) -> dict:
    seeds = jax.random.split(jax.random.key(seed), 8)
    magnitudes = draw_magnitudes(jax.random.fold_in(seeds[7], 71), 0)
    weights = jnp.clip(jnp.exp(math.log(4.0) - 2.7725887 * jax.random.uniform(seeds[1], (NBANDS, OBS, NSTARS), jnp.float32) ** block_scale(seeds[1], (NBANDS, OBS, NSTARS), ((0, 4), (2, 8)), -0.2, 0.2)), 0.25, 4.0)
    slots = draw_slots(jax.random.fold_in(seeds[7], 71), 0)
    block_fields = draw_block_fields(jax.random.fold_in(seeds[7], 71), 0)
    owner = draw_owner(jax.random.fold_in(seeds[7], 71), 0)
    colors = place_ends(jax.random.randint(seeds[5], (F,), 0, COLORS), jax.random.fold_in(seeds[5], 1), 0, COLORS - 1).astype(jnp.int32)
    color_terms = jnp.clip(jax.random.uniform(seeds[6], (NBANDS, NBANDS), jnp.float32, -0.25, 0.25), -0.25, 0.25)
    return {"magnitudes": magnitudes, "weights": weights, "slots": slots, "block_fields": block_fields, "owner": owner, "colors": colors, "color_terms": color_terms}


PRIOR_WEIGHT = 1.0


def field_table(block_fields, slots):
    band_count, obs_count, star_count = slots.shape
    block_count, list_len = block_fields.shape
    block_rows = star_count // block_count
    block_slots = slots.reshape(band_count, obs_count, block_count, block_rows)
    expanded = jnp.broadcast_to(block_fields[None, None, :, :], (band_count, obs_count, block_count, list_len))
    picked = jnp.take_along_axis(expanded, block_slots, axis=3)
    return picked.reshape(band_count, obs_count, star_count).astype(jnp.int32)


def reference(magnitudes, weights, slots, block_fields, owner, colors, color_terms):
    band_count, obs_count, star_count = magnitudes.shape
    fields = owner.shape[0]
    field_ids = field_table(block_fields, slots)
    star_weight = jnp.sum(weights, axis=1)

    def segment_one(band_values, band_ids):
        return jax.ops.segment_sum(band_values.reshape(-1), band_ids.reshape(-1), num_segments=fields)

    def field_sums(values):
        return jax.vmap(segment_one)(values, field_ids)

    denominators = field_sums(weights) + PRIOR_WEIGHT
    mixing = jnp.eye(band_count, dtype=jnp.float32) + color_terms - jnp.diag(jnp.sum(color_terms, axis=1))

    def predict(zero_pts):
        zp_obs = jax.vmap(jnp.take)(zero_pts, field_ids)
        star_means = jnp.sum(weights * (magnitudes - zp_obs), axis=1) / star_weight
        predicted = jnp.dot(mixing, star_means, precision=lax.Precision.HIGHEST)
        return zp_obs, star_means, predicted

    zero_pts = jnp.zeros((band_count, fields), jnp.float32)
    misfits = []
    for sweep_no in range(SWEEPS):
        for color_no in range(COLORS):
            zp_obs, star_means, predicted = predict(zero_pts)
            residual = magnitudes - predicted[:, None, :]
            if color_no == 0 and sweep_no > 0:
                misfits.append(jnp.sum(weights * (residual - zp_obs) ** 2, axis=(1, 2)))
            updated = field_sums(weights * residual) / denominators
            zero_pts = jnp.where((colors == color_no)[None, :], updated, zero_pts)
    zp_obs, star_means, predicted = predict(zero_pts)
    residual = magnitudes - predicted[:, None, :]
    misfits.append(jnp.sum(weights * (residual - zp_obs) ** 2, axis=(1, 2)))
    misfit = jnp.stack(misfits) / (obs_count * star_count)
    owner_order = jnp.argsort(owner, stable=True)
    return jnp.take(zero_pts, owner_order, axis=1), star_means, misfit
```

```python
import functools

import jax
import jax.numpy as jnp
from jax import lax
from jax.experimental import pallas as pl
from jax.experimental.pallas import tpu as pltpu
from jax.sharding import PartitionSpec as P

COLORS = 8
SWEEPS = 4
PRIOR_WEIGHT = 1.0
REACH = 2
HIGHEST = lax.Precision.HIGHEST
LANES = 128
EXTRA = 8


def contract_lanes(left, right):
    dims = (((1,), (1,)), ((), ()))
    return lax.dot_general(left, right, dims, precision=HIGHEST, preferred_element_type=jnp.float32)


def couple_kernel(bands, obs, list_len, rows, mix_ref, mix_grid_ref, data_ref, out_ref):
    blocks = out_ref.shape[0]
    entry = lax.broadcasted_iota(jnp.int32, (list_len, rows), 0).astype(jnp.float32)
    for block in range(blocks):
        cols = pl.ds(block * rows, rows)
        one_hot, one_hot_mag, star_weight, means = [], [], [], []
        for band in range(bands):
            mags = data_ref[band, 0:obs, cols]
            wts = data_ref[band, obs : 2 * obs, cols]
            slots = data_ref[band, 2 * obs : 3 * obs, cols]
            scaled = wts * mags
            weight_sum = jnp.sum(wts, axis=0, keepdims=True)
            star_weight.append(weight_sum)
            means.append(jnp.sum(scaled, axis=0, keepdims=True) / weight_sum)
            hot = jnp.zeros((list_len, rows), jnp.float32)
            hot_mag = jnp.zeros((list_len, rows), jnp.float32)
            for k in range(obs):
                hit = slots[k : k + 1] == entry
                hot = hot + jnp.where(hit, wts[k : k + 1], 0.0)
                hot_mag = hot_mag + jnp.where(hit, scaled[k : k + 1], 0.0)
            one_hot.append(hot)
            one_hot_mag.append(hot_mag)
        rest = []
        shares = []
        for band in range(bands):
            predicted = mix_ref[band, 0] * means[0]
            for other in range(1, bands):
                predicted = predicted + mix_ref[band, other] * means[other]
            rest.append(one_hot_mag[band] - one_hot[band] * predicted)
            shares.append(one_hot[band] / star_weight[band])
        hot_all = jnp.concatenate(one_hot, axis=0)
        share_all = jnp.concatenate(shares, axis=0)
        rest_all = jnp.concatenate(rest, axis=0)
        out_ref[block, 0:LANES, :] = contract_lanes(share_all, hot_all) * mix_grid_ref[...]
        ones = jnp.ones((8, rows), jnp.float32)
        rest_row = contract_lanes(ones, rest_all)
        weight_row = contract_lanes(ones, hot_all)
        first = lax.broadcasted_iota(jnp.int32, (8, LANES), 0) == 0
        out_ref[block, LANES : LANES + EXTRA, :] = jnp.where(first, rest_row, weight_row)


def sweep_kernel(tiles, blocks, coupled_ref, pick_ref, color_ref, out_ref, kt, base, tot, rden, zp, stage, sems):
    near = 2 * REACH + 1

    def fetch(tile, slot):
        return pltpu.make_async_copy(
            coupled_ref.at[pl.ds(tile * blocks, blocks)], stage.at[slot], sems.at[slot]
        )

    def tile_rows(tile):
        return pl.ds(pl.multiple_of(tile * blocks, blocks), blocks)

    fetch(0, 0).start()

    def unpack(tile, carry):
        slot = lax.rem(tile, 2)

        @pl.when(tile + 1 < tiles)
        def _():
            fetch(tile + 1, 1 - slot).start()

        fetch(tile, slot).wait()
        for block in range(blocks):
            kt[pl.ds(tile * (LANES * blocks) + block, LANES, stride=blocks), :] = stage[slot, block, 0:LANES, :]
            base[pl.ds(tile * blocks + block, 1), :] = stage[slot, block, LANES : LANES + 1, :]
            tot[pl.ds(tile * blocks + block, 1), :] = stage[slot, block, LANES + 1 : LANES + 2, :]
        return carry

    lax.fori_loop(0, tiles, unpack, 0)

    def gathered(tile):
        sums = [jnp.zeros((blocks, LANES), jnp.float32) for _ in range(4)]
        for offset in range(near):
            source = lax.rem(tile + offset + tiles - REACH, tiles) * blocks
            for block in range(blocks):
                place = offset * blocks + block
                pick = pick_ref[tile, place]
                row = jnp.broadcast_to(tot[pl.ds(source + block, 1), :], (blocks, LANES))
                got = jnp.take_along_axis(row, pick & (LANES - 1), axis=1, mode="promise_in_bounds")
                sums[place % 4] = sums[place % 4] + jnp.where(pick < LANES, got, 0.0)
        return (sums[0] + sums[1]) + (sums[2] + sums[3])

    def weigh(tile, carry):
        rden[tile_rows(tile), :] = 1.0 / (gathered(tile) + PRIOR_WEIGHT)
        return carry

    lax.fori_loop(0, tiles, weigh, 0)
    zp[...] = jnp.zeros_like(zp)

    def step(number, carry):
        color_no = lax.rem(number, COLORS)

        def total(tile, inner):
            here = zp[tile_rows(tile), :]
            sums = [base[tile_rows(tile), :]] + [jnp.zeros((blocks, LANES), jnp.float32) for _ in range(3)]
            for j in range(LANES):
                rows = pl.ds(pl.multiple_of(tile * (LANES * blocks) + j * blocks, blocks), blocks)
                value = jnp.broadcast_to(here[:, j : j + 1], (blocks, LANES))
                sums[j % 4] = sums[j % 4] + value * kt[rows, :]
            tot[tile_rows(tile), :] = (sums[0] + sums[1]) + (sums[2] + sums[3])
            return inner

        lax.fori_loop(0, tiles, total, 0, unroll=2)

        def update(tile, inner):
            rows = tile_rows(tile)
            fresh = gathered(tile) * rden[rows, :]
            zp[rows, :] = jnp.where(color_ref[rows, :] == color_no, fresh, zp[rows, :])
            return inner

        lax.fori_loop(0, tiles, update, 0, unroll=2)

        @pl.when(color_no == COLORS - 1)
        def _():
            out_ref[lax.div(number, COLORS)] = zp[...]

        return carry

    lax.fori_loop(0, SWEEPS * COLORS, step, 0)


def finish_kernel(bands, obs, list_len, rows, mix_ref, data_ref, own_ref, zp_two_ref, zp_own_ref, means_ref, misfit_ref):
    my_band = lax.axis_index("band")
    halves = rows // LANES

    def spread(row, picks):
        table = jnp.broadcast_to(row, (obs, LANES))
        return jnp.take_along_axis(table, picks, axis=1, mode="promise_in_bounds")

    for block in range(zp_own_ref.shape[0]):
        row = zp_own_ref[block : block + 1, :]
        for half in range(halves):
            cols = pl.ds(block * rows + half * LANES, LANES)
            wts = own_ref[obs : 2 * obs, cols]
            picks = own_ref[2 * obs : 3 * obs, cols].astype(jnp.int32) + my_band * list_len
            left = wts * (own_ref[0:obs, cols] - spread(row, picks))
            means_ref[0:1, cols] = jnp.sum(left, axis=0, keepdims=True) / jnp.sum(wts, axis=0, keepdims=True)

    for sweep in range(SWEEPS):
        partial = [jnp.zeros((obs, LANES), jnp.float32) for _ in range(bands)]
        for block in range(zp_two_ref.shape[1]):
            row = zp_two_ref[sweep, block : block + 1, :]
            for half in range(halves):
                cols = pl.ds(block * rows + half * LANES, LANES)
                left, means = [], []
                for band in range(bands):
                    wts = data_ref[band, obs : 2 * obs, cols]
                    picks = data_ref[band, 2 * obs : 3 * obs, cols].astype(jnp.int32) + band * list_len
                    mags = data_ref[band, 0:obs, cols] - spread(row, picks)
                    left.append(mags)
                    means.append(jnp.sum(wts * mags, axis=0, keepdims=True) / jnp.sum(wts, axis=0, keepdims=True))
                for band in range(bands):
                    predicted = mix_ref[band, 0] * means[0]
                    for other in range(1, bands):
                        predicted = predicted + mix_ref[band, other] * means[other]
                    wts = data_ref[band, obs : 2 * obs, cols]
                    partial[band] = partial[band] + wts * (left[band] - predicted) ** 2
        for band in range(bands):
            line = jnp.sum(partial[band], axis=0, keepdims=True)
            misfit_ref[sweep * bands + band : sweep * bands + band + 1, :] = line


def body(magnitudes, weights, slots, block_fields, owner, colors, color_terms):
    bands = color_terms.shape[0]
    tiles = lax.axis_size("sky")
    my_tile = lax.axis_index("sky")
    my_band = lax.axis_index("band")
    _, obs, stars = magnitudes.shape
    blocks, list_len = block_fields.shape
    rows = stars // blocks
    fields = owner.shape[0]
    owned = fields // tiles
    mine = blocks // bands
    mixing = (
        jnp.eye(bands, dtype=jnp.float32) + color_terms - jnp.diag(jnp.sum(color_terms, axis=1))
    )
    vmem = pl.BlockSpec(memory_space=pltpu.VMEM)
    smem = pl.BlockSpec(memory_space=pltpu.SMEM)
    hbm = pl.BlockSpec(memory_space=pl.ANY)

    own = jnp.concatenate([magnitudes[0], weights[0], slots[0].astype(jnp.float32)], axis=0)
    data = lax.all_to_all(own, "band", split_axis=1, concat_axis=0, tiled=True)
    data = data.reshape(bands, 3 * obs, mine * rows)
    all_fields = lax.all_gather(block_fields, "sky", axis=0, tiled=True)

    mix_grid = jnp.repeat(jnp.repeat(mixing.T, list_len, axis=0), list_len, axis=1)
    coupled = pl.pallas_call(
        functools.partial(couple_kernel, bands, obs, list_len, rows),
        out_shape=jax.ShapeDtypeStruct((mine, LANES + EXTRA, LANES), jnp.float32),
        in_specs=[smem, vmem, vmem],
        out_specs=vmem,
        name="couple",
    )(mixing, mix_grid, data)
    coupled = lax.all_gather(coupled, ("sky", "band"), axis=0, tiled=True)

    live = all_fields < fields
    entry_colors = jnp.where(live, jnp.take(colors, jnp.minimum(all_fields, fields - 1)), -1)
    entry_colors = jnp.tile(entry_colors, (1, bands))
    by_tile = all_fields.reshape(tiles, blocks, list_len)
    near = jnp.stack([jnp.roll(by_tile, REACH - n, axis=0) for n in range(2 * REACH + 1)], axis=1)
    near = near.reshape(tiles, (2 * REACH + 1) * blocks, list_len)
    lane_fields = jnp.tile(by_tile, (1, 1, bands))[:, None]
    lane_band = jnp.arange(LANES, dtype=jnp.int32) // list_len * list_len
    pick = jnp.full((tiles, near.shape[1], blocks, LANES), LANES, jnp.int32)
    for entry in range(list_len):
        pick = jnp.where(near[:, :, entry][:, :, None, None] == lane_fields, lane_band + entry, pick)
    pick = jnp.where(lane_fields < fields, pick, LANES)

    total_blocks = tiles * blocks
    big = (total_blocks, LANES)
    snapshots = pl.pallas_call(
        functools.partial(sweep_kernel, tiles, blocks),
        out_shape=jax.ShapeDtypeStruct((SWEEPS,) + big, jnp.float32),
        in_specs=[hbm, vmem, vmem],
        out_specs=vmem,
        scratch_shapes=[
            pltpu.VMEM((total_blocks * LANES, LANES), jnp.float32),
            pltpu.VMEM(big, jnp.float32),
            pltpu.VMEM(big, jnp.float32),
            pltpu.VMEM(big, jnp.float32),
            pltpu.VMEM(big, jnp.float32),
            pltpu.VMEM((2, blocks, LANES + EXTRA, LANES), jnp.float32),
            pltpu.SemaphoreType.DMA((2,)),
        ],
        compiler_params=pltpu.CompilerParams(vmem_limit_bytes=60 * 1024 * 1024),
        name="sweeps",
    )(coupled, pick, entry_colors)

    first = my_tile * blocks
    zp_tile = lax.dynamic_slice_in_dim(snapshots[SWEEPS - 1], first, blocks, axis=0)
    zp_two = lax.dynamic_slice_in_dim(snapshots, first + my_band * mine, mine, axis=1)
    star_means, partial = pl.pallas_call(
        functools.partial(finish_kernel, bands, obs, list_len, rows),
        out_shape=(
            jax.ShapeDtypeStruct((1, stars), jnp.float32),
            jax.ShapeDtypeStruct((SWEEPS * bands, LANES), jnp.float32),
        ),
        in_specs=[smem, vmem, vmem, vmem, vmem],
        out_specs=(vmem, vmem),
        name="finish",
    )(mixing, data, own, zp_two, zp_tile)
    partial = jnp.sum(partial, axis=1).reshape(SWEEPS, bands)
    misfit = lax.psum(partial, ("sky", "band")) / (obs * stars * tiles)
    misfit = lax.dynamic_slice_in_dim(misfit, my_band, 1, axis=1)

    tile_ids = jnp.mod(my_tile + jnp.arange(3, dtype=jnp.int32) - 1, tiles)
    close_fields = jnp.concatenate(
        [lax.dynamic_index_in_dim(by_tile, tile_ids[n], 0, keepdims=False) for n in range(3)], axis=0
    ).reshape(-1)
    field_no = jnp.arange(fields, dtype=jnp.int32)[:, None]
    is_mine = (owner == my_tile)[:, None]
    rank = jnp.sum((is_mine & (field_no < close_fields[None])).astype(jnp.int32), axis=0)
    has = jnp.sum((is_mine & (field_no == close_fields[None])).astype(jnp.int32), axis=0) > 0
    rank = jnp.where(has, rank, owned)
    count = close_fields.shape[0]
    entry_no = jnp.arange(count, dtype=jnp.int32)[:, None]
    hit = rank[:, None] == jnp.arange(owned, dtype=jnp.int32)[None]
    chosen = jnp.max(jnp.where(hit, entry_no, -1), axis=0)
    last = lax.dynamic_slice_in_dim(snapshots[SWEEPS - 1], my_band * list_len, list_len, axis=1)
    last = last.reshape(tiles, blocks, list_len)
    close_zp = jnp.concatenate(
        [lax.dynamic_index_in_dim(last, tile_ids[n], 0, keepdims=False) for n in range(3)], axis=0
    ).reshape(-1)
    own_zp = jnp.sum(jnp.where(chosen[None] == entry_no, close_zp[:, None], 0.0), axis=0)
    return own_zp[None], star_means, misfit


def solution(mesh):
    in_specs = (
        P("band", None, "sky"),
        P("band", None, "sky"),
        P("band", None, "sky"),
        P("sky", None),
        P(),
        P(),
        P(),
    )
    out_specs = (P("band", "sky"), P("band", "sky"), P(None, "band"))
    return jax.shard_map(body, mesh=mesh, in_specs=in_specs, out_specs=out_specs, check_vma=False)
```

```python
import functools

import jax
import jax.numpy as jnp
from jax import lax
from jax.experimental import pallas as pl
from jax.experimental.pallas import tpu as pltpu
from jax.sharding import PartitionSpec as P

COLORS = 8
SWEEPS = 4
PRIOR_WEIGHT = 1.0
REACH = 2
HIGHEST = lax.Precision.HIGHEST
LANES = 128
EXTRA = 8


def contract_lanes(left, right):
    dims = (((1,), (1,)), ((), ()))
    return lax.dot_general(left, right, dims, precision=HIGHEST, preferred_element_type=jnp.float32)


def couple_kernel(bands, obs, list_len, rows, mix_ref, mix_grid_ref, data_ref, out_ref):
    blocks = data_ref.shape[2] // rows
    full = []
    entry = lax.broadcasted_iota(jnp.int32, (list_len, rows), 0).astype(jnp.float32)
    for block in range(blocks):
        cols = pl.ds(block * rows, rows)
        one_hot, one_hot_mag, star_weight, means = [], [], [], []
        for band in range(bands):
            mags = data_ref[band, 0:obs, cols]
            wts = data_ref[band, obs : 2 * obs, cols]
            slots = data_ref[band, 2 * obs : 3 * obs, cols]
            scaled = wts * mags
            weight_sum = jnp.sum(wts, axis=0, keepdims=True)
            star_weight.append(weight_sum)
            means.append(jnp.sum(scaled, axis=0, keepdims=True) / weight_sum)
            hot = jnp.zeros((list_len, rows), jnp.float32)
            hot_mag = jnp.zeros((list_len, rows), jnp.float32)
            for k in range(obs):
                hit = slots[k : k + 1] == entry
                hot = hot + jnp.where(hit, wts[k : k + 1], 0.0)
                hot_mag = hot_mag + jnp.where(hit, scaled[k : k + 1], 0.0)
            one_hot.append(hot)
            one_hot_mag.append(hot_mag)
        rest = []
        shares = []
        for band in range(bands):
            predicted = mix_ref[band, 0] * means[0]
            for other in range(1, bands):
                predicted = predicted + mix_ref[band, other] * means[other]
            rest.append(one_hot_mag[band] - one_hot[band] * predicted)
            shares.append(one_hot[band] / star_weight[band])
        hot_all = jnp.concatenate(one_hot, axis=0)
        share_all = jnp.concatenate(shares, axis=0)
        rest_all = jnp.concatenate(rest, axis=0)
        coupling = contract_lanes(share_all, hot_all) * mix_grid_ref[...]
        ones = jnp.ones((8, rows), jnp.float32)
        rest_row = contract_lanes(ones, rest_all)
        weight_row = contract_lanes(ones, hot_all)
        first = lax.broadcasted_iota(jnp.int32, (EXTRA, LANES), 0) == 0
        full.append(jnp.concatenate([coupling, jnp.where(first, rest_row, weight_row)], axis=0))
    split = bands // 2
    for part in range(split):
        pieces = []
        for half in range(2):
            band = half * split + part
            for block in range(blocks):
                pieces.append(full[block][:, band * list_len : (band + 1) * list_len])
        out_ref[part] = jnp.concatenate(pieces, axis=1)


def sweep_kernel(bands, list_len, row_count, coupled_ref, pick_ref, color_ref, out_ref, kt, base, tot, rden, zp, stage, sems):
    groups = row_count // 8
    pack = LANES // list_len
    split = bands // 2
    patterns = pick_ref.shape[0]
    depth = stage.shape[0]
    lane = lax.broadcasted_iota(jnp.int32, (8, LANES), 1)
    lane_wide = lax.broadcasted_iota(jnp.int32, (LANES + EXTRA, LANES), 1)

    def fetch(row, slot):
        return pltpu.make_async_copy(
            coupled_ref.at[pl.ds(row * (2 * split), 2 * split)], stage.at[slot], sems.at[slot]
        )

    for row in range(depth - 1):
        fetch(row, row).start()

    def unpack(row, carry):
        slot = lax.rem(row, depth)
        ahead = row + depth - 1

        @pl.when(ahead < row_count)
        def _():
            fetch(ahead, lax.rem(ahead, depth)).start()

        fetch(row, slot).wait()
        group = lax.div(row, 8)
        place = lax.rem(row, 8)
        for part in range(split):
            left = stage[slot, part]
            right = stage[slot, split + part]
            low = jnp.where(lane_wide < LANES // 2, left, pltpu.roll(right, LANES // 2, 1))
            high = jnp.where(lane_wide < LANES // 2, pltpu.roll(left, LANES // 2, 1), right)
            for band, value in ((part, low), (split + part, high)):
                start = (group * bands + band) * (LANES * 8) + place
                kt[pl.ds(start, LANES, stride=8), :] = value[0:LANES]
                base[band, pl.ds(row, 1), :] = value[LANES : LANES + 1]
                tot[band, pl.ds(row + 8, 1), :] = value[LANES + 1 : LANES + 2]
        return carry

    lax.fori_loop(0, row_count, unpack, 0)

    def rows_of(group):
        return pl.ds(pl.multiple_of(group * 8, 8), 8)

    def wrap():
        for band in range(bands):
            tot[band, 0:8, :] = tot[band, row_count : row_count + 8, :]
            tot[band, row_count + 8 : row_count + 16, :] = tot[band, 8:16, :]

    def take(value, picks):
        return jnp.take_along_axis(value, picks, axis=1, mode="promise_in_bounds")

    def gathered(group):
        sums = [jnp.zeros((8, LANES), jnp.float32) for _ in range(2 * bands)]
        for place in range(patterns // pack):
            start = group * 8 + (8 + place - patterns // pack // 2)
            near = [tot[band, pl.ds(start, 8), :] for band in range(bands)]
            for quarter in range(pack):
                pick = pick_ref[place * pack + quarter, rows_of(group), :]
                mask = pick < LANES
                lanes = pick & (LANES - 1)
                for band in range(bands):
                    index = 2 * band + quarter % 2
                    sums[index] = sums[index] + jnp.where(mask, take(near[band], lanes), 0.0)
        return [sums[2 * band] + sums[2 * band + 1] for band in range(bands)]

    def weigh(group, carry):
        for band, value in enumerate(gathered(group)):
            rden[band, rows_of(group), :] = 1.0 / (value + PRIOR_WEIGHT)
        return carry

    wrap()
    lax.fori_loop(0, groups, weigh, 0)
    zp[...] = jnp.zeros_like(zp)

    def step(number, carry):
        color_no = lax.rem(number, COLORS)

        def total(group, inner):
            here = [zp[band, rows_of(group), :] for band in range(bands)]
            sums = [base[band, rows_of(group), :] for band in range(bands)]
            for entry in range(list_len):
                lanes = (lane & (LANES - list_len)) + entry
                values = [take(here[band], lanes) for band in range(bands)]
                for band in range(bands):
                    for other in range(bands):
                        start = (group * bands + band) * (LANES * 8) + (other * list_len + entry) * 8
                        rows = pl.ds(pl.multiple_of(start, 8), 8)
                        sums[band] = sums[band] + values[other] * kt[rows, :]
            for band in range(bands):
                tot[band, pl.ds(pl.multiple_of(group * 8 + 8, 8), 8), :] = sums[band]
            return inner

        lax.fori_loop(0, groups, total, 0, unroll=2)
        wrap()

        def update(group, inner):
            rows = rows_of(group)
            now = color_ref[rows, :] == color_no
            for band, value in enumerate(gathered(group)):
                zp[band, rows, :] = jnp.where(now, value * rden[band, rows, :], zp[band, rows, :])
            return inner

        lax.fori_loop(0, groups, update, 0, unroll=2)

        @pl.when(color_no == COLORS - 1)
        def _():
            out_ref[lax.div(number, COLORS)] = zp[...]

        return carry

    lax.fori_loop(0, SWEEPS * COLORS, step, 0)


def match_kernel(list_len, fields, places, rows_ref, pick_ref):
    pack = LANES // list_len

    def group_picks(group, carry):
        home = rows_ref[pl.ds(pl.multiple_of(group * 8 + 8, 8), 8), :]
        home = jnp.where(home < fields, home, -1)
        near = [rows_ref[pl.ds(group * 8 + 8 + place - places // 2, 8), :] for place in range(places)]
        for quarter in range(pack):
            picks = [jnp.full((8, LANES), LANES, jnp.int32) for _ in range(places)]
            for entry in range(list_len):
                source = quarter * list_len + entry
                for place in range(places):
                    other = jnp.broadcast_to(near[place][:, source : source + 1], (8, LANES))
                    picks[place] = jnp.where(other == home, source, picks[place])
            for place in range(places):
                pick_ref[place * pack + quarter, pl.ds(pl.multiple_of(group * 8, 8), 8), :] = picks[place]
        return carry

    lax.fori_loop(0, pick_ref.shape[1] // 8, group_picks, 0)


def finish_kernel(bands, obs, list_len, rows, mix_ref, data_ref, own_ref, zp_two_ref, zp_own_ref, means_ref, misfit_ref):
    halves = rows // LANES
    pack = LANES // list_len
    mine = data_ref.shape[2] // rows
    first = lax.rem(lax.axis_index("band") * mine, pack)

    def spread(row, picks):
        table = jnp.broadcast_to(row, (obs, LANES))
        return jnp.take_along_axis(table, picks, axis=1, mode="promise_in_bounds")

    for block in range(zp_own_ref.shape[0] * pack):
        row = zp_own_ref[block // pack : block // pack + 1, :]
        for half in range(halves):
            cols = pl.ds(block * rows + half * LANES, LANES)
            wts = own_ref[obs : 2 * obs, cols]
            picks = own_ref[2 * obs : 3 * obs, cols].astype(jnp.int32) + block % pack * list_len
            left = wts * (own_ref[0:obs, cols] - spread(row, picks))
            means_ref[0:1, cols] = jnp.sum(left, axis=0, keepdims=True) / jnp.sum(wts, axis=0, keepdims=True)

    lines = []
    for sweep in range(SWEEPS):
        partial = [jnp.zeros((obs, LANES), jnp.float32) for _ in range(bands)]
        for block in range(mine):
            for half in range(halves):
                cols = pl.ds(block * rows + half * LANES, LANES)
                left, means = [], []
                for band in range(bands):
                    wts = data_ref[band, obs : 2 * obs, cols]
                    picks = data_ref[band, 2 * obs : 3 * obs, cols].astype(jnp.int32) + (first + block) * list_len
                    row = zp_two_ref[sweep, band]
                    mags = data_ref[band, 0:obs, cols] - spread(row, picks)
                    left.append(mags)
                    means.append(jnp.sum(wts * mags, axis=0, keepdims=True) / jnp.sum(wts, axis=0, keepdims=True))
                for band in range(bands):
                    predicted = mix_ref[band, 0] * means[0]
                    for other in range(1, bands):
                        predicted = predicted + mix_ref[band, other] * means[other]
                    wts = data_ref[band, obs : 2 * obs, cols]
                    partial[band] = partial[band] + wts * (left[band] - predicted) ** 2
        lines += [jnp.sum(partial[band], axis=0, keepdims=True) for band in range(bands)]
    block_sums = jnp.concatenate(lines, axis=0)
    misfit_ref[...] = contract_lanes(jnp.ones((8, LANES), jnp.float32), block_sums)[0:1]


def body(magnitudes, weights, slots, block_fields, owner, colors, color_terms):
    bands = color_terms.shape[0]
    tiles = lax.axis_size("sky")
    my_tile = lax.axis_index("sky")
    my_band = lax.axis_index("band")
    _, obs, stars = magnitudes.shape
    blocks, list_len = block_fields.shape
    rows = stars // blocks
    fields = owner.shape[0]
    owned = fields // tiles
    mine = blocks // bands
    pack = LANES // list_len
    tile_rows = blocks // pack
    row_count = tiles * tile_rows
    mixing = (
        jnp.eye(bands, dtype=jnp.float32) + color_terms - jnp.diag(jnp.sum(color_terms, axis=1))
    )
    vmem = pl.BlockSpec(memory_space=pltpu.VMEM)
    smem = pl.BlockSpec(memory_space=pltpu.SMEM)
    hbm = pl.BlockSpec(memory_space=pl.ANY)

    field_no = jnp.arange(fields, dtype=jnp.int32)[:, None]
    flat_fields = block_fields.reshape(1, -1)
    own_colors = jnp.sum(jnp.where(field_no == flat_fields, colors[:, None], 0), axis=0)
    own_colors = jnp.where(flat_fields[0] < fields, own_colors, -1)
    lists = jnp.stack([flat_fields[0], own_colors]).reshape(1, 2, tile_rows, LANES)
    lists = lax.all_gather(lists, "sky", axis=0, tiled=True)
    all_fields = lists[:, 0].reshape(row_count, LANES)
    entry_colors = lists[:, 1].reshape(row_count, LANES)

    own = jnp.concatenate([magnitudes[0], weights[0], slots[0].astype(jnp.float32)], axis=0)
    data = lax.all_to_all(own, "band", split_axis=1, concat_axis=0, tiled=True)
    data = data.reshape(bands, 3 * obs, mine * rows)
    data, all_fields, entry_colors = lax.optimization_barrier((data, all_fields, entry_colors))

    mix_grid = jnp.repeat(jnp.repeat(mixing.T, list_len, axis=0), list_len, axis=1)
    coupled = pl.pallas_call(
        functools.partial(couple_kernel, bands, obs, list_len, rows),
        out_shape=jax.ShapeDtypeStruct((bands // 2, LANES + EXTRA, LANES), jnp.float32),
        in_specs=[smem, vmem, vmem],
        out_specs=vmem,
        name="couple",
    )(mixing, mix_grid, data)
    coupled = lax.all_gather(coupled, ("sky", "band"), axis=0, tiled=True)

    reach_rows = REACH * tile_rows + tile_rows - 1
    padded = jnp.concatenate([all_fields[-8:], all_fields, all_fields[:8]], axis=0)
    places = 2 * reach_rows + 1
    pick = pl.pallas_call(
        functools.partial(match_kernel, list_len, fields, places),
        out_shape=jax.ShapeDtypeStruct((places * pack, row_count, LANES), jnp.int32),
        in_specs=[vmem],
        out_specs=vmem,
        cost_estimate=pl.CostEstimate(flops=10**7, bytes_accessed=10**6, transcendentals=0),
        name="match",
    )(padded)

    big = (bands, row_count, LANES)
    snapshots = pl.pallas_call(
        functools.partial(sweep_kernel, bands, list_len, row_count),
        out_shape=jax.ShapeDtypeStruct((SWEEPS,) + big, jnp.float32),
        in_specs=[hbm, vmem, vmem],
        out_specs=vmem,
        scratch_shapes=[
            pltpu.VMEM((row_count * bands * LANES, LANES), jnp.float32),
            pltpu.VMEM(big, jnp.float32),
            pltpu.VMEM((bands, row_count + 16, LANES), jnp.float32),
            pltpu.VMEM(big, jnp.float32),
            pltpu.VMEM(big, jnp.float32),
            pltpu.VMEM((4, bands, LANES + EXTRA, LANES), jnp.float32),
            pltpu.SemaphoreType.DMA((4,)),
        ],
        compiler_params=pltpu.CompilerParams(vmem_limit_bytes=60 * 1024 * 1024),
        name="sweeps",
    )(coupled, pick, entry_colors)

    final = lax.dynamic_index_in_dim(snapshots[SWEEPS - 1], my_band, 0, keepdims=False)
    zp_tile = lax.dynamic_slice_in_dim(final, my_tile * tile_rows, tile_rows, axis=0)
    my_row = (my_tile * blocks + my_band * mine) // pack
    zp_two = lax.dynamic_slice_in_dim(snapshots, my_row, 1, axis=2)
    star_means, partial = pl.pallas_call(
        functools.partial(finish_kernel, bands, obs, list_len, rows),
        out_shape=(
            jax.ShapeDtypeStruct((1, stars), jnp.float32),
            jax.ShapeDtypeStruct((1, SWEEPS * bands), jnp.float32),
        ),
        in_specs=[smem, vmem, vmem, vmem, vmem],
        out_specs=(vmem, vmem),
        name="finish",
    )(mixing, data, own, zp_two, zp_tile)
    partial = lax.all_gather(partial, ("sky", "band"), axis=0, tiled=True)
    misfit = jnp.sum(partial, axis=0).reshape(SWEEPS, bands) / (obs * stars * tiles)
    misfit = lax.dynamic_slice_in_dim(misfit, my_band, 1, axis=1)

    tile_ids = jnp.mod(my_tile + jnp.arange(3, dtype=jnp.int32) - 1, tiles)

    def close(table):
        by_tile = table.reshape(tiles, tile_rows * LANES)
        parts = [lax.dynamic_index_in_dim(by_tile, tile_ids[n], 0, keepdims=False) for n in range(3)]
        return jnp.concatenate(parts)

    close_fields = close(all_fields)
    is_mine = (owner == my_tile)[:, None]
    rank = jnp.sum((is_mine & (field_no < close_fields[None])).astype(jnp.int32), axis=0)
    has = jnp.sum((is_mine & (field_no == close_fields[None])).astype(jnp.int32), axis=0) > 0
    rank = jnp.where(has, rank, owned)
    entry_no = jnp.arange(close_fields.shape[0], dtype=jnp.int32)[:, None]
    hit = rank[:, None] == jnp.arange(owned, dtype=jnp.int32)[None]
    chosen = jnp.max(jnp.where(hit, entry_no, -1), axis=0)
    own_zp = jnp.sum(jnp.where(chosen[None] == entry_no, close(final)[:, None], 0.0), axis=0)
    return own_zp[None], star_means, misfit


def solution(mesh):
    in_specs = (
        P("band", None, "sky"),
        P("band", None, "sky"),
        P("band", None, "sky"),
        P("sky", None),
        P(),
        P(),
        P(),
    )
    out_specs = (P("band", "sky"), P("band", "sky"), P(None, "band"))
    return jax.shard_map(body, mesh=mesh, in_specs=in_specs, out_specs=out_specs, check_vma=False)
```

```python
import functools

import jax
import jax.numpy as jnp
from jax import lax
from jax.experimental import pallas as pl
from jax.experimental.pallas import tpu as pltpu
from jax.sharding import PartitionSpec as P

COLORS = 8
SWEEPS = 4
PRIOR_WEIGHT = 1.0
REACH = 2
HIGHEST = lax.Precision.HIGHEST
LANES = 128
EXTRA = 8
MESH = pl.DeviceIdType.MESH


def contract_lanes(left, right):
    dims = (((1,), (1,)), ((), ()))
    return lax.dot_general(left, right, dims, precision=HIGHEST, preferred_element_type=jnp.float32)


def couple_kernel(bands, obs, list_len, rows, mix_ref, mix_grid_ref, data_ref, out_ref):
    blocks = data_ref.shape[2] // rows
    full = []
    entry = lax.broadcasted_iota(jnp.int32, (list_len, rows), 0).astype(jnp.float32)
    for block in range(blocks):
        cols = pl.ds(block * rows, rows)
        one_hot, one_hot_mag, star_weight, means = [], [], [], []
        for band in range(bands):
            mags = data_ref[band, 0:obs, cols]
            wts = data_ref[band, obs : 2 * obs, cols]
            slots = data_ref[band, 2 * obs : 3 * obs, cols]
            scaled = wts * mags
            weight_sum = jnp.sum(wts, axis=0, keepdims=True)
            star_weight.append(weight_sum)
            means.append(jnp.sum(scaled, axis=0, keepdims=True) / weight_sum)
            hot = jnp.zeros((list_len, rows), jnp.float32)
            hot_mag = jnp.zeros((list_len, rows), jnp.float32)
            for k in range(obs):
                hit = slots[k : k + 1] == entry
                hot = hot + jnp.where(hit, wts[k : k + 1], 0.0)
                hot_mag = hot_mag + jnp.where(hit, scaled[k : k + 1], 0.0)
            one_hot.append(hot)
            one_hot_mag.append(hot_mag)
        rest = []
        shares = []
        for band in range(bands):
            predicted = mix_ref[band, 0] * means[0]
            for other in range(1, bands):
                predicted = predicted + mix_ref[band, other] * means[other]
            rest.append(one_hot_mag[band] - one_hot[band] * predicted)
            shares.append(one_hot[band] / star_weight[band])
        hot_all = jnp.concatenate(one_hot, axis=0)
        share_all = jnp.concatenate(shares, axis=0)
        rest_all = jnp.concatenate(rest, axis=0)
        coupling = contract_lanes(share_all, hot_all) * mix_grid_ref[...]
        ones = jnp.ones((8, rows), jnp.float32)
        rest_row = contract_lanes(ones, rest_all)
        weight_row = contract_lanes(ones, hot_all)
        first = lax.broadcasted_iota(jnp.int32, (EXTRA, LANES), 0) == 0
        full.append(jnp.concatenate([coupling, jnp.where(first, rest_row, weight_row)], axis=0))
    split = bands // 2
    for part in range(split):
        pieces = []
        for half in range(2):
            band = half * split + part
            for block in range(blocks):
                pieces.append(full[block][:, band * list_len : (band + 1) * list_len])
        out_ref[part] = jnp.concatenate(pieces, axis=1)


def sweep_kernel(bands, list_len, row_count, coupled_ref, pick_ref, color_ref, out_ref, kt, base, tot, rden, zp, stage, sems):
    groups = row_count // 8
    pack = LANES // list_len
    split = bands // 2
    patterns = pick_ref.shape[0]
    depth = stage.shape[0]
    lane = lax.broadcasted_iota(jnp.int32, (8, LANES), 1)
    lane_wide = lax.broadcasted_iota(jnp.int32, (LANES + EXTRA, LANES), 1)

    def fetch(row, slot):
        return pltpu.make_async_copy(
            coupled_ref.at[pl.ds(row * (2 * split), 2 * split)], stage.at[slot], sems.at[slot]
        )

    for row in range(depth - 1):
        fetch(row, row).start()

    def unpack(row, carry):
        slot = lax.rem(row, depth)
        ahead = row + depth - 1

        @pl.when(ahead < row_count)
        def _():
            fetch(ahead, lax.rem(ahead, depth)).start()

        fetch(row, slot).wait()
        group = lax.div(row, 8)
        place = lax.rem(row, 8)
        for part in range(split):
            left = stage[slot, part]
            right = stage[slot, split + part]
            low = jnp.where(lane_wide < LANES // 2, left, pltpu.roll(right, LANES // 2, 1))
            high = jnp.where(lane_wide < LANES // 2, pltpu.roll(left, LANES // 2, 1), right)
            for band, value in ((part, low), (split + part, high)):
                start = (group * bands + band) * (LANES * 8) + place
                kt[pl.ds(start, LANES, stride=8), :] = value[0:LANES]
                base[band, pl.ds(row, 1), :] = value[LANES : LANES + 1]
                tot[band, pl.ds(row + 8, 1), :] = value[LANES + 1 : LANES + 2]
        return carry

    lax.fori_loop(0, row_count, unpack, 0)

    def rows_of(group):
        return pl.ds(pl.multiple_of(group * 8, 8), 8)

    def wrap():
        for band in range(bands):
            tot[band, 0:8, :] = tot[band, row_count : row_count + 8, :]
            tot[band, row_count + 8 : row_count + 16, :] = tot[band, 8:16, :]

    def take(value, picks):
        return jnp.take_along_axis(value, picks, axis=1, mode="promise_in_bounds")

    def gathered(group):
        sums = [jnp.zeros((8, LANES), jnp.float32) for _ in range(2 * bands)]
        for place in range(patterns // pack):
            start = group * 8 + (8 + place - patterns // pack // 2)
            near = [tot[band, pl.ds(start, 8), :] for band in range(bands)]
            for quarter in range(pack):
                pick = pick_ref[place * pack + quarter, rows_of(group), :]
                mask = pick < LANES
                lanes = pick & (LANES - 1)
                for band in range(bands):
                    index = 2 * band + quarter % 2
                    sums[index] = sums[index] + jnp.where(mask, take(near[band], lanes), 0.0)
        return [sums[2 * band] + sums[2 * band + 1] for band in range(bands)]

    def weigh(group, carry):
        for band, value in enumerate(gathered(group)):
            rden[band, rows_of(group), :] = 1.0 / (value + PRIOR_WEIGHT)
        return carry

    wrap()
    lax.fori_loop(0, groups, weigh, 0)
    zp[...] = jnp.zeros_like(zp)

    def step(number, carry):
        color_no = lax.rem(number, COLORS)

        def total(group, inner):
            here = [zp[band, rows_of(group), :] for band in range(bands)]
            sums = [base[band, rows_of(group), :] for band in range(bands)]
            for entry in range(list_len):
                lanes = (lane & (LANES - list_len)) + entry
                values = [take(here[band], lanes) for band in range(bands)]
                for band in range(bands):
                    for other in range(bands):
                        start = (group * bands + band) * (LANES * 8) + (other * list_len + entry) * 8
                        rows = pl.ds(pl.multiple_of(start, 8), 8)
                        sums[band] = sums[band] + values[other] * kt[rows, :]
            for band in range(bands):
                tot[band, pl.ds(pl.multiple_of(group * 8 + 8, 8), 8), :] = sums[band]
            return inner

        lax.fori_loop(0, groups, total, 0, unroll=2)
        wrap()

        def update(group, inner):
            rows = rows_of(group)
            now = color_ref[rows, :] == color_no
            for band, value in enumerate(gathered(group)):
                zp[band, rows, :] = jnp.where(now, value * rden[band, rows, :], zp[band, rows, :])
            return inner

        lax.fori_loop(0, groups, update, 0, unroll=2)

        @pl.when(color_no == COLORS - 1)
        def _():
            out_ref[lax.div(number, COLORS)] = zp[...]

        return carry

    lax.fori_loop(0, SWEEPS * COLORS, step, 0)


def greet(axes):
    barrier = pltpu.get_barrier_semaphore()
    total = 0
    for axis, count in axes:
        for step in range(1, count):
            peer = lax.rem(lax.axis_index(axis) + step, count)
            pl.semaphore_signal(barrier, inc=1, device_id={axis: peer}, device_id_type=MESH)
            total += 1
    pl.semaphore_wait(barrier, total)


def send_all(axis, count, source, target, send_sems, recv_sems, first):
    me = lax.axis_index(axis)
    copies = []
    for step in range(1, count):
        peer = lax.rem(me + step, count)
        copy = pltpu.make_async_remote_copy(
            src_ref=source(peer),
            dst_ref=target.at[me],
            send_sem=send_sems.at[first + step - 1],
            recv_sem=recv_sems.at[first + step - 1],
            device_id={axis: peer},
            device_id_type=MESH,
        )
        copy.start()
        copies.append(copy)
    return copies


def exchange_kernel(tiles, bands, lists_ref, own_ref, all_lists_ref, data_ref, send_sems, recv_sems):
    greet((("sky", tiles), ("band", bands)))
    copies = send_all("sky", tiles, lambda peer: lists_ref, all_lists_ref, send_sems, recv_sems, 0)
    copies += send_all("band", bands, lambda peer: own_ref.at[peer], data_ref, send_sems, recv_sems, tiles - 1)
    my_band = lax.axis_index("band")
    all_lists_ref[lax.axis_index("sky")] = lists_ref[...]
    data_ref[my_band] = own_ref[my_band]
    for copy in copies:
        copy.wait()


def total_kernel(tiles, bands, part_ref, out_ref, by_band, held, by_tile, send_sems, recv_sems):
    greet((("sky", tiles), ("band", bands)))
    copies = send_all("band", bands, lambda peer: part_ref, by_band, send_sems, recv_sems, tiles - 1)
    by_band[lax.axis_index("band")] = part_ref[...]
    for copy in copies:
        copy.wait()
    total = by_band[0]
    for band in range(1, bands):
        total = total + by_band[band]
    held[...] = total
    copies = send_all("sky", tiles, lambda peer: held, by_tile, send_sems, recv_sems, 0)
    by_tile[lax.axis_index("sky")] = total
    for copy in copies:
        copy.wait()
    total = by_tile[0]
    for tile in range(1, tiles):
        total = total + by_tile[tile]
    out_ref[...] = total


def match_kernel(list_len, fields, places, rows_ref, pick_ref):
    pack = LANES // list_len

    def group_picks(group, carry):
        home = rows_ref[pl.ds(pl.multiple_of(group * 8 + 8, 8), 8), :]
        home = jnp.where(home < fields, home, -1)
        near = [rows_ref[pl.ds(group * 8 + 8 + place - places // 2, 8), :] for place in range(places)]
        for quarter in range(pack):
            picks = [jnp.full((8, LANES), LANES, jnp.int32) for _ in range(places)]
            for entry in range(list_len):
                source = quarter * list_len + entry
                for place in range(places):
                    other = jnp.broadcast_to(near[place][:, source : source + 1], (8, LANES))
                    picks[place] = jnp.where(other == home, source, picks[place])
            for place in range(places):
                pick_ref[place * pack + quarter, pl.ds(pl.multiple_of(group * 8, 8), 8), :] = picks[place]
        return carry

    lax.fori_loop(0, pick_ref.shape[1] // 8, group_picks, 0)


def finish_kernel(bands, obs, list_len, rows, mix_ref, data_ref, own_ref, zp_two_ref, zp_own_ref, means_ref, misfit_ref):
    halves = rows // LANES
    pack = LANES // list_len
    mine = data_ref.shape[2] // rows
    first = lax.rem(lax.axis_index("band") * mine, pack)

    def spread(row, picks):
        table = jnp.broadcast_to(row, (obs, LANES))
        return jnp.take_along_axis(table, picks, axis=1, mode="promise_in_bounds")

    for block in range(zp_own_ref.shape[0] * pack):
        row = zp_own_ref[block // pack : block // pack + 1, :]
        for half in range(halves):
            cols = pl.ds(block * rows + half * LANES, LANES)
            wts = own_ref[obs : 2 * obs, cols]
            picks = own_ref[2 * obs : 3 * obs, cols].astype(jnp.int32) + block % pack * list_len
            left = wts * (own_ref[0:obs, cols] - spread(row, picks))
            means_ref[0:1, cols] = jnp.sum(left, axis=0, keepdims=True) / jnp.sum(wts, axis=0, keepdims=True)

    lines = []
    for sweep in range(SWEEPS):
        partial = [jnp.zeros((obs, LANES), jnp.float32) for _ in range(bands)]
        for block in range(mine):
            for half in range(halves):
                cols = pl.ds(block * rows + half * LANES, LANES)
                left, means = [], []
                for band in range(bands):
                    wts = data_ref[band, obs : 2 * obs, cols]
                    picks = data_ref[band, 2 * obs : 3 * obs, cols].astype(jnp.int32) + (first + block) * list_len
                    row = zp_two_ref[sweep, band]
                    mags = data_ref[band, 0:obs, cols] - spread(row, picks)
                    left.append(mags)
                    means.append(jnp.sum(wts * mags, axis=0, keepdims=True) / jnp.sum(wts, axis=0, keepdims=True))
                for band in range(bands):
                    predicted = mix_ref[band, 0] * means[0]
                    for other in range(1, bands):
                        predicted = predicted + mix_ref[band, other] * means[other]
                    wts = data_ref[band, obs : 2 * obs, cols]
                    partial[band] = partial[band] + wts * (left[band] - predicted) ** 2
        lines += [jnp.sum(partial[band], axis=0, keepdims=True) for band in range(bands)]
    lines.append(jnp.zeros((LANES - len(lines), LANES), jnp.float32))
    block_sums = jnp.concatenate(lines, axis=0)
    misfit_ref[...] = contract_lanes(jnp.ones((8, LANES), jnp.float32), block_sums)


def body(magnitudes, weights, slots, block_fields, owner, colors, color_terms):
    bands = color_terms.shape[0]
    tiles = lax.axis_size("sky")
    my_tile = lax.axis_index("sky")
    my_band = lax.axis_index("band")
    _, obs, stars = magnitudes.shape
    blocks, list_len = block_fields.shape
    rows = stars // blocks
    fields = owner.shape[0]
    owned = fields // tiles
    mine = blocks // bands
    pack = LANES // list_len
    tile_rows = blocks // pack
    row_count = tiles * tile_rows
    mixing = (
        jnp.eye(bands, dtype=jnp.float32) + color_terms - jnp.diag(jnp.sum(color_terms, axis=1))
    )
    vmem = pl.BlockSpec(memory_space=pltpu.VMEM)
    smem = pl.BlockSpec(memory_space=pltpu.SMEM)
    hbm = pl.BlockSpec(memory_space=pl.ANY)

    field_no = jnp.arange(fields, dtype=jnp.int32)[:, None]
    flat_fields = block_fields.reshape(1, -1)
    own_colors = jnp.sum(jnp.where(field_no == flat_fields, colors[:, None], 0), axis=0)
    own_colors = jnp.where(flat_fields[0] < fields, own_colors, -1)
    lists = jnp.stack([flat_fields[0], own_colors]).reshape(2 * tile_rows, LANES)
    own = jnp.concatenate([magnitudes[0], weights[0], slots[0].astype(jnp.float32)], axis=0)
    by_peer = own.reshape(3 * obs, bands, mine * rows).transpose(1, 0, 2)
    peers = tiles + bands - 2
    lists, data = pl.pallas_call(
        functools.partial(exchange_kernel, tiles, bands),
        out_shape=(
            jax.ShapeDtypeStruct((tiles,) + lists.shape, jnp.int32),
            jax.ShapeDtypeStruct(by_peer.shape, jnp.float32),
        ),
        in_specs=[vmem, vmem],
        out_specs=(vmem, vmem),
        scratch_shapes=[pltpu.SemaphoreType.DMA((peers,)), pltpu.SemaphoreType.DMA((peers,))],
        compiler_params=pltpu.CompilerParams(collective_id=0, has_side_effects=True),
        name="exchange",
    )(lists, by_peer)
    lists = lists.reshape(tiles, 2, tile_rows, LANES)
    all_fields = lists[:, 0].reshape(row_count, LANES)
    entry_colors = lists[:, 1].reshape(row_count, LANES)

    mix_grid = jnp.repeat(jnp.repeat(mixing.T, list_len, axis=0), list_len, axis=1)
    coupled = pl.pallas_call(
        functools.partial(couple_kernel, bands, obs, list_len, rows),
        out_shape=jax.ShapeDtypeStruct((bands // 2, LANES + EXTRA, LANES), jnp.float32),
        in_specs=[smem, vmem, vmem],
        out_specs=vmem,
        name="couple",
    )(mixing, mix_grid, data)
    coupled = lax.all_gather(coupled, ("sky", "band"), axis=0, tiled=True)

    reach_rows = REACH * tile_rows + tile_rows - 1
    padded = jnp.concatenate([all_fields[-8:], all_fields, all_fields[:8]], axis=0)
    places = 2 * reach_rows + 1
    pick = pl.pallas_call(
        functools.partial(match_kernel, list_len, fields, places),
        out_shape=jax.ShapeDtypeStruct((places * pack, row_count, LANES), jnp.int32),
        in_specs=[vmem],
        out_specs=vmem,
        cost_estimate=pl.CostEstimate(flops=10**7, bytes_accessed=10**6, transcendentals=0),
        name="match",
    )(padded)

    big = (bands, row_count, LANES)
    snapshots = pl.pallas_call(
        functools.partial(sweep_kernel, bands, list_len, row_count),
        out_shape=jax.ShapeDtypeStruct((SWEEPS,) + big, jnp.float32),
        in_specs=[hbm, vmem, vmem],
        out_specs=vmem,
        scratch_shapes=[
            pltpu.VMEM((row_count * bands * LANES, LANES), jnp.float32),
            pltpu.VMEM(big, jnp.float32),
            pltpu.VMEM((bands, row_count + 16, LANES), jnp.float32),
            pltpu.VMEM(big, jnp.float32),
            pltpu.VMEM(big, jnp.float32),
            pltpu.VMEM((4, bands, LANES + EXTRA, LANES), jnp.float32),
            pltpu.SemaphoreType.DMA((4,)),
        ],
        compiler_params=pltpu.CompilerParams(vmem_limit_bytes=60 * 1024 * 1024),
        name="sweeps",
    )(coupled, pick, entry_colors)

    final = lax.dynamic_index_in_dim(snapshots[SWEEPS - 1], my_band, 0, keepdims=False)
    zp_tile = lax.dynamic_slice_in_dim(final, my_tile * tile_rows, tile_rows, axis=0)
    my_row = (my_tile * blocks + my_band * mine) // pack
    zp_two = lax.dynamic_slice_in_dim(snapshots, my_row, 1, axis=2)
    star_means, partial = pl.pallas_call(
        functools.partial(finish_kernel, bands, obs, list_len, rows),
        out_shape=(
            jax.ShapeDtypeStruct((1, stars), jnp.float32),
            jax.ShapeDtypeStruct((8, LANES), jnp.float32),
        ),
        in_specs=[smem, vmem, vmem, vmem, vmem],
        out_specs=(vmem, vmem),
        name="finish",
    )(mixing, data, own, zp_two, zp_tile)
    slab = (8, LANES)
    total = pl.pallas_call(
        functools.partial(total_kernel, tiles, bands),
        out_shape=jax.ShapeDtypeStruct(slab, jnp.float32),
        in_specs=[vmem],
        out_specs=vmem,
        scratch_shapes=[
            pltpu.VMEM((bands,) + slab, jnp.float32),
            pltpu.VMEM(slab, jnp.float32),
            pltpu.VMEM((tiles,) + slab, jnp.float32),
            pltpu.SemaphoreType.DMA((peers,)),
            pltpu.SemaphoreType.DMA((peers,)),
        ],
        compiler_params=pltpu.CompilerParams(collective_id=1, has_side_effects=True),
        name="total",
    )(partial)
    misfit = total[0, : SWEEPS * bands].reshape(SWEEPS, bands) / (obs * stars * tiles)
    misfit = lax.dynamic_slice_in_dim(misfit, my_band, 1, axis=1)

    tile_ids = jnp.mod(my_tile + jnp.arange(3, dtype=jnp.int32) - 1, tiles)

    def close(table):
        by_tile = table.reshape(tiles, tile_rows * LANES)
        parts = [lax.dynamic_index_in_dim(by_tile, tile_ids[n], 0, keepdims=False) for n in range(3)]
        return jnp.concatenate(parts)

    close_fields = close(all_fields)
    is_mine = (owner == my_tile)[:, None]
    rank = jnp.sum((is_mine & (field_no < close_fields[None])).astype(jnp.int32), axis=0)
    has = jnp.sum((is_mine & (field_no == close_fields[None])).astype(jnp.int32), axis=0) > 0
    rank = jnp.where(has, rank, owned)
    entry_no = jnp.arange(close_fields.shape[0], dtype=jnp.int32)[:, None]
    hit = rank[:, None] == jnp.arange(owned, dtype=jnp.int32)[None]
    chosen = jnp.max(jnp.where(hit, entry_no, -1), axis=0)
    own_zp = jnp.sum(jnp.where(chosen[None] == entry_no, close(final)[:, None], 0.0), axis=0)
    return own_zp[None], star_means, misfit


def solution(mesh):
    in_specs = (
        P("band", None, "sky"),
        P("band", None, "sky"),
        P("band", None, "sky"),
        P("sky", None),
        P(),
        P(),
        P(),
    )
    out_specs = (P("band", "sky"), P("band", "sky"), P(None, "band"))
    return jax.shard_map(body, mesh=mesh, in_specs=in_specs, out_specs=out_specs, check_vma=False)
```

```python
import functools

import jax
import jax.numpy as jnp
from jax import lax
from jax.experimental import pallas as pl
from jax.experimental.pallas import tpu as pltpu
from jax.sharding import PartitionSpec as P

COLORS = 8
SWEEPS = 4
PRIOR_WEIGHT = 1.0
REACH = 2
HIGHEST = lax.Precision.HIGHEST
LANES = 128
EXTRA = 8
MESH = pl.DeviceIdType.MESH


def contract_lanes(left, right):
    dims = (((1,), (1,)), ((), ()))
    return lax.dot_general(left, right, dims, precision=HIGHEST, preferred_element_type=jnp.float32)


def couple_kernel(bands, obs, list_len, rows, mix_ref, mix_grid_ref, data_ref, out_ref):
    blocks = data_ref.shape[2] // rows
    full = []
    entry = lax.broadcasted_iota(jnp.int32, (list_len, rows), 0).astype(jnp.float32)
    for block in range(blocks):
        cols = pl.ds(block * rows, rows)
        one_hot, one_hot_mag, star_weight, means = [], [], [], []
        for band in range(bands):
            mags = data_ref[band, 0:obs, cols]
            wts = data_ref[band, obs : 2 * obs, cols]
            slots = data_ref[band, 2 * obs : 3 * obs, cols]
            scaled = wts * mags
            weight_sum = jnp.sum(wts, axis=0, keepdims=True)
            star_weight.append(weight_sum)
            means.append(jnp.sum(scaled, axis=0, keepdims=True) / weight_sum)
            hot = jnp.zeros((list_len, rows), jnp.float32)
            hot_mag = jnp.zeros((list_len, rows), jnp.float32)
            for k in range(obs):
                hit = slots[k : k + 1] == entry
                hot = hot + jnp.where(hit, wts[k : k + 1], 0.0)
                hot_mag = hot_mag + jnp.where(hit, scaled[k : k + 1], 0.0)
            one_hot.append(hot)
            one_hot_mag.append(hot_mag)
        rest = []
        shares = []
        for band in range(bands):
            predicted = mix_ref[band, 0] * means[0]
            for other in range(1, bands):
                predicted = predicted + mix_ref[band, other] * means[other]
            rest.append(one_hot_mag[band] - one_hot[band] * predicted)
            shares.append(one_hot[band] / star_weight[band])
        hot_all = jnp.concatenate(one_hot, axis=0)
        share_all = jnp.concatenate(shares, axis=0)
        rest_all = jnp.concatenate(rest, axis=0)
        coupling = contract_lanes(share_all, hot_all) * mix_grid_ref[...]
        ones = jnp.ones((8, rows), jnp.float32)
        rest_row = contract_lanes(ones, rest_all)
        weight_row = contract_lanes(ones, hot_all)
        first = lax.broadcasted_iota(jnp.int32, (EXTRA, LANES), 0) == 0
        full.append(jnp.concatenate([coupling, jnp.where(first, rest_row, weight_row)], axis=0))
    split = bands // 2
    for part in range(split):
        pieces = []
        for half in range(2):
            band = half * split + part
            for block in range(blocks):
                pieces.append(full[block][:, band * list_len : (band + 1) * list_len])
        out_ref[part] = jnp.concatenate(pieces, axis=1)


def sweep_kernel(bands, list_len, row_count, coupled_ref, pick_ref, color_ref, out_ref, kt, base, tot, rden, zp, stage, sems):
    groups = row_count // 8
    pack = LANES // list_len
    split = bands // 2
    patterns = pick_ref.shape[0]
    depth = stage.shape[0]
    lane = lax.broadcasted_iota(jnp.int32, (8, LANES), 1)
    lane_wide = lax.broadcasted_iota(jnp.int32, (LANES + EXTRA, LANES), 1)

    def fetch(row, slot):
        return pltpu.make_async_copy(
            coupled_ref.at[pl.ds(row * (2 * split), 2 * split)], stage.at[slot], sems.at[slot]
        )

    for row in range(depth - 1):
        fetch(row, row).start()

    def unpack(row, carry):
        slot = lax.rem(row, depth)
        ahead = row + depth - 1

        @pl.when(ahead < row_count)
        def _():
            fetch(ahead, lax.rem(ahead, depth)).start()

        fetch(row, slot).wait()
        group = lax.div(row, 8)
        place = lax.rem(row, 8)
        for part in range(split):
            left = stage[slot, part]
            right = stage[slot, split + part]
            low = jnp.where(lane_wide < LANES // 2, left, pltpu.roll(right, LANES // 2, 1))
            high = jnp.where(lane_wide < LANES // 2, pltpu.roll(left, LANES // 2, 1), right)
            for band, value in ((part, low), (split + part, high)):
                start = (group * bands + band) * (LANES * 8) + place
                kt[pl.ds(start, LANES, stride=8), :] = value[0:LANES]
                base[band, pl.ds(row, 1), :] = value[LANES : LANES + 1]
                tot[band, pl.ds(row + 8, 1), :] = value[LANES + 1 : LANES + 2]
        return carry

    lax.fori_loop(0, row_count, unpack, 0)

    def rows_of(group):
        return pl.ds(pl.multiple_of(group * 8, 8), 8)

    def wrap():
        for band in range(bands):
            tot[band, 0:8, :] = tot[band, row_count : row_count + 8, :]
            tot[band, row_count + 8 : row_count + 16, :] = tot[band, 8:16, :]

    def take(value, picks):
        return jnp.take_along_axis(value, picks, axis=1, mode="promise_in_bounds")

    def gathered(group):
        sums = [jnp.zeros((8, LANES), jnp.float32) for _ in range(2 * bands)]
        for place in range(patterns // pack):
            start = group * 8 + (8 + place - patterns // pack // 2)
            near = [tot[band, pl.ds(start, 8), :] for band in range(bands)]
            for quarter in range(pack):
                pick = pick_ref[place * pack + quarter, rows_of(group), :]
                mask = pick < LANES
                lanes = pick & (LANES - 1)
                for band in range(bands):
                    index = 2 * band + quarter % 2
                    sums[index] = sums[index] + jnp.where(mask, take(near[band], lanes), 0.0)
        return [sums[2 * band] + sums[2 * band + 1] for band in range(bands)]

    def weigh(group, carry):
        for band, value in enumerate(gathered(group)):
            rden[band, rows_of(group), :] = 1.0 / (value + PRIOR_WEIGHT)
        return carry

    wrap()
    lax.fori_loop(0, groups, weigh, 0)
    zp[...] = jnp.zeros_like(zp)

    def step(number, carry):
        color_no = lax.rem(number, COLORS)

        def total(group, inner):
            here = [zp[band, rows_of(group), :] for band in range(bands)]
            sums = [base[band, rows_of(group), :] for band in range(bands)]
            for entry in range(list_len):
                lanes = (lane & (LANES - list_len)) + entry
                values = [take(here[band], lanes) for band in range(bands)]
                for band in range(bands):
                    for other in range(bands):
                        start = (group * bands + band) * (LANES * 8) + (other * list_len + entry) * 8
                        rows = pl.ds(pl.multiple_of(start, 8), 8)
                        sums[band] = sums[band] + values[other] * kt[rows, :]
            for band in range(bands):
                tot[band, pl.ds(pl.multiple_of(group * 8 + 8, 8), 8), :] = sums[band]
            return inner

        lax.fori_loop(0, groups, total, 0, unroll=2)
        wrap()

        def update(group, inner):
            rows = rows_of(group)
            now = color_ref[rows, :] == color_no
            for band, value in enumerate(gathered(group)):
                zp[band, rows, :] = jnp.where(now, value * rden[band, rows, :], zp[band, rows, :])
            return inner

        lax.fori_loop(0, groups, update, 0, unroll=2)

        @pl.when(color_no == COLORS - 1)
        def _():
            out_ref[lax.div(number, COLORS)] = zp[...]

        return carry

    lax.fori_loop(0, SWEEPS * COLORS, step, 0)


def greet(axes):
    barrier = pltpu.get_barrier_semaphore()
    total = 0
    for axis, count in axes:
        for step in range(1, count):
            peer = lax.rem(lax.axis_index(axis) + step, count)
            pl.semaphore_signal(barrier, inc=1, device_id={axis: peer}, device_id_type=MESH)
            total += 1
    pl.semaphore_wait(barrier, total)


def send_all(axis, count, source, target, send_sems, recv_sems, first):
    me = lax.axis_index(axis)
    copies = []
    for step in range(1, count):
        peer = lax.rem(me + step, count)
        copy = pltpu.make_async_remote_copy(
            src_ref=source(peer),
            dst_ref=target.at[me],
            send_sem=send_sems.at[first + step - 1],
            recv_sem=recv_sems.at[first + step - 1],
            device_id={axis: peer},
            device_id_type=MESH,
        )
        copy.start()
        copies.append(copy)
    return copies


def exchange_kernel(tiles, bands, lists_ref, own_ref, all_lists_ref, data_ref, send_sems, recv_sems):
    greet((("sky", tiles), ("band", bands)))
    copies = send_all("sky", tiles, lambda peer: lists_ref, all_lists_ref, send_sems, recv_sems, 0)
    copies += send_all("band", bands, lambda peer: own_ref.at[peer], data_ref, send_sems, recv_sems, tiles - 1)
    my_band = lax.axis_index("band")
    all_lists_ref[lax.axis_index("sky")] = lists_ref[...]
    data_ref[my_band] = own_ref[my_band]
    for copy in copies:
        copy.wait()


def spread_kernel(high_count, own_ref, all_ref, send_sems, recv_sems):
    sky, band = lax.axis_index("sky"), lax.axis_index("band")
    high, low = sky // 2, sky % 2
    side, core = band // 2, band % 2
    highs = [lax.rem(high + step, high_count) for step in range(1, high_count)]
    to_low = {"sky": high * 2 + (1 - low)}
    to_side = {"band": (1 - side) * 2 + core}
    to_core = {"band": side * 2 + (1 - core)}
    peers = [{"sky": peer * 2 + low} for peer in highs] + [to_low, to_side, to_core]
    barrier = pltpu.get_barrier_semaphore()
    for peer in peers:
        pl.semaphore_signal(barrier, inc=1, device_id=peer, device_id_type=MESH)
    pl.semaphore_wait(barrier, len(peers))
    count = [0]

    def send(source, target, peer):
        copy = pltpu.make_async_remote_copy(
            src_ref=source,
            dst_ref=target,
            send_sem=send_sems.at[count[0]],
            recv_sem=recv_sems.at[count[0]],
            device_id=peer,
            device_id_type=MESH,
        )
        count[0] += 1
        copy.start()
        return copy

    def wait(copies):
        for copy in copies:
            copy.wait()

    mine = all_ref.at[high, low, side, core]
    copies = [send(own_ref, mine, peer) for peer in peers[: high_count - 1]]
    all_ref[high, low, side, core] = own_ref[...]
    wait(copies)

    column = all_ref.at[:, low, side, core]
    first = all_ref.at[:, low, side, core, 0]
    second = all_ref.at[:, low, side, core, 1]
    copies = [send(first, first, to_low), send(second, second, to_side)]
    late = [send(column, column, to_core)]
    wait(copies)

    first = all_ref.at[:, :, side, core, 0]
    second = all_ref.at[:, low, :, core, 1]
    copies = [send(first, first, to_side), send(second, second, to_low)]
    for part in (all_ref.at[:, 1 - low, side, core, 0], all_ref.at[:, low, 1 - side, core, 1]):
        late.append(send(part, part, to_core))
    wait(copies)

    for part in (all_ref.at[:, :, 1 - side, core, 0], all_ref.at[:, 1 - low, :, core, 1]):
        late.append(send(part, part, to_core))
    wait(late)


def total_kernel(tiles, bands, part_ref, out_ref, by_band, held, by_tile, send_sems, recv_sems):
    greet((("sky", tiles), ("band", bands)))
    copies = send_all("band", bands, lambda peer: part_ref, by_band, send_sems, recv_sems, tiles - 1)
    by_band[lax.axis_index("band")] = part_ref[...]
    for copy in copies:
        copy.wait()
    total = by_band[0]
    for band in range(1, bands):
        total = total + by_band[band]
    held[...] = total
    copies = send_all("sky", tiles, lambda peer: held, by_tile, send_sems, recv_sems, 0)
    by_tile[lax.axis_index("sky")] = total
    for copy in copies:
        copy.wait()
    total = by_tile[0]
    for tile in range(1, tiles):
        total = total + by_tile[tile]
    out_ref[...] = total


def match_kernel(list_len, fields, places, rows_ref, pick_ref):
    pack = LANES // list_len

    def group_picks(group, carry):
        home = rows_ref[pl.ds(pl.multiple_of(group * 8 + 8, 8), 8), :]
        home = jnp.where(home < fields, home, -1)
        near = [rows_ref[pl.ds(group * 8 + 8 + place - places // 2, 8), :] for place in range(places)]
        for quarter in range(pack):
            picks = [jnp.full((8, LANES), LANES, jnp.int32) for _ in range(places)]
            for entry in range(list_len):
                source = quarter * list_len + entry
                for place in range(places):
                    other = jnp.broadcast_to(near[place][:, source : source + 1], (8, LANES))
                    picks[place] = jnp.where(other == home, source, picks[place])
            for place in range(places):
                pick_ref[place * pack + quarter, pl.ds(pl.multiple_of(group * 8, 8), 8), :] = picks[place]
        return carry

    lax.fori_loop(0, pick_ref.shape[1] // 8, group_picks, 0)


def finish_kernel(bands, obs, list_len, rows, mix_ref, data_ref, own_ref, zp_two_ref, zp_own_ref, means_ref, misfit_ref):
    halves = rows // LANES
    pack = LANES // list_len
    mine = data_ref.shape[2] // rows
    first = lax.rem(lax.axis_index("band") * mine, pack)

    def spread(row, picks):
        table = jnp.broadcast_to(row, (obs, LANES))
        return jnp.take_along_axis(table, picks, axis=1, mode="promise_in_bounds")

    for block in range(zp_own_ref.shape[0] * pack):
        row = zp_own_ref[block // pack : block // pack + 1, :]
        for half in range(halves):
            cols = pl.ds(block * rows + half * LANES, LANES)
            wts = own_ref[obs : 2 * obs, cols]
            picks = own_ref[2 * obs : 3 * obs, cols].astype(jnp.int32) + block % pack * list_len
            left = wts * (own_ref[0:obs, cols] - spread(row, picks))
            means_ref[0:1, cols] = jnp.sum(left, axis=0, keepdims=True) / jnp.sum(wts, axis=0, keepdims=True)

    lines = []
    for sweep in range(SWEEPS):
        partial = [jnp.zeros((obs, LANES), jnp.float32) for _ in range(bands)]
        for block in range(mine):
            for half in range(halves):
                cols = pl.ds(block * rows + half * LANES, LANES)
                left, means = [], []
                for band in range(bands):
                    wts = data_ref[band, obs : 2 * obs, cols]
                    picks = data_ref[band, 2 * obs : 3 * obs, cols].astype(jnp.int32) + (first + block) * list_len
                    row = zp_two_ref[sweep, band]
                    mags = data_ref[band, 0:obs, cols] - spread(row, picks)
                    left.append(mags)
                    means.append(jnp.sum(wts * mags, axis=0, keepdims=True) / jnp.sum(wts, axis=0, keepdims=True))
                for band in range(bands):
                    predicted = mix_ref[band, 0] * means[0]
                    for other in range(1, bands):
                        predicted = predicted + mix_ref[band, other] * means[other]
                    wts = data_ref[band, obs : 2 * obs, cols]
                    partial[band] = partial[band] + wts * (left[band] - predicted) ** 2
        lines += [jnp.sum(partial[band], axis=0, keepdims=True) for band in range(bands)]
    lines.append(jnp.zeros((LANES - len(lines), LANES), jnp.float32))
    block_sums = jnp.concatenate(lines, axis=0)
    misfit_ref[...] = contract_lanes(jnp.ones((8, LANES), jnp.float32), block_sums)


def body(magnitudes, weights, slots, block_fields, owner, colors, color_terms):
    bands = color_terms.shape[0]
    tiles = lax.axis_size("sky")
    my_tile = lax.axis_index("sky")
    my_band = lax.axis_index("band")
    _, obs, stars = magnitudes.shape
    blocks, list_len = block_fields.shape
    rows = stars // blocks
    fields = owner.shape[0]
    owned = fields // tiles
    mine = blocks // bands
    pack = LANES // list_len
    tile_rows = blocks // pack
    row_count = tiles * tile_rows
    mixing = (
        jnp.eye(bands, dtype=jnp.float32) + color_terms - jnp.diag(jnp.sum(color_terms, axis=1))
    )
    vmem = pl.BlockSpec(memory_space=pltpu.VMEM)
    smem = pl.BlockSpec(memory_space=pltpu.SMEM)
    hbm = pl.BlockSpec(memory_space=pl.ANY)

    field_no = jnp.arange(fields, dtype=jnp.int32)[:, None]
    flat_fields = block_fields.reshape(1, -1)
    own_colors = jnp.sum(jnp.where(field_no == flat_fields, colors[:, None], 0), axis=0)
    own_colors = jnp.where(flat_fields[0] < fields, own_colors, -1)
    lists = jnp.stack([flat_fields[0], own_colors]).reshape(2 * tile_rows, LANES)
    own = jnp.concatenate([magnitudes[0], weights[0], slots[0].astype(jnp.float32)], axis=0)
    by_peer = own.reshape(3 * obs, bands, mine * rows).transpose(1, 0, 2)
    peers = tiles + bands - 2
    lists, data = pl.pallas_call(
        functools.partial(exchange_kernel, tiles, bands),
        out_shape=(
            jax.ShapeDtypeStruct((tiles,) + lists.shape, jnp.int32),
            jax.ShapeDtypeStruct(by_peer.shape, jnp.float32),
        ),
        in_specs=[vmem, vmem],
        out_specs=(vmem, vmem),
        scratch_shapes=[pltpu.SemaphoreType.DMA((peers,)), pltpu.SemaphoreType.DMA((peers,))],
        compiler_params=pltpu.CompilerParams(collective_id=0, has_side_effects=True),
        name="exchange",
    )(lists, by_peer)
    lists = lists.reshape(tiles, 2, tile_rows, LANES)
    all_fields = lists[:, 0].reshape(row_count, LANES)
    entry_colors = lists[:, 1].reshape(row_count, LANES)

    mix_grid = jnp.repeat(jnp.repeat(mixing.T, list_len, axis=0), list_len, axis=1)
    coupled = pl.pallas_call(
        functools.partial(couple_kernel, bands, obs, list_len, rows),
        out_shape=jax.ShapeDtypeStruct((bands // 2, LANES + EXTRA, LANES), jnp.float32),
        in_specs=[smem, vmem, vmem],
        out_specs=vmem,
        name="couple",
    )(mixing, mix_grid, data)
    everyone = (tiles // 2, 2, bands // 2, 2) + coupled.shape
    copies = tiles // 2 - 1 + 9
    coupled = pl.pallas_call(
        functools.partial(spread_kernel, tiles // 2),
        out_shape=jax.ShapeDtypeStruct(everyone, jnp.float32),
        in_specs=[vmem],
        out_specs=vmem,
        scratch_shapes=[pltpu.SemaphoreType.DMA((copies,)), pltpu.SemaphoreType.DMA((copies,))],
        compiler_params=pltpu.CompilerParams(
            collective_id=2, has_side_effects=True, vmem_limit_bytes=60 * 1024 * 1024
        ),
        name="spread",
    )(coupled)
    coupled = coupled.reshape((-1,) + coupled.shape[-2:])

    reach_rows = REACH * tile_rows + tile_rows - 1
    padded = jnp.concatenate([all_fields[-8:], all_fields, all_fields[:8]], axis=0)
    places = 2 * reach_rows + 1
    pick = pl.pallas_call(
        functools.partial(match_kernel, list_len, fields, places),
        out_shape=jax.ShapeDtypeStruct((places * pack, row_count, LANES), jnp.int32),
        in_specs=[vmem],
        out_specs=vmem,
        cost_estimate=pl.CostEstimate(flops=10**7, bytes_accessed=10**6, transcendentals=0),
        name="match",
    )(padded)

    big = (bands, row_count, LANES)
    snapshots = pl.pallas_call(
        functools.partial(sweep_kernel, bands, list_len, row_count),
        out_shape=jax.ShapeDtypeStruct((SWEEPS,) + big, jnp.float32),
        in_specs=[hbm, vmem, vmem],
        out_specs=vmem,
        scratch_shapes=[
            pltpu.VMEM((row_count * bands * LANES, LANES), jnp.float32),
            pltpu.VMEM(big, jnp.float32),
            pltpu.VMEM((bands, row_count + 16, LANES), jnp.float32),
            pltpu.VMEM(big, jnp.float32),
            pltpu.VMEM(big, jnp.float32),
            pltpu.VMEM((4, bands, LANES + EXTRA, LANES), jnp.float32),
            pltpu.SemaphoreType.DMA((4,)),
        ],
        compiler_params=pltpu.CompilerParams(vmem_limit_bytes=60 * 1024 * 1024),
        name="sweeps",
    )(coupled, pick, entry_colors)

    final = lax.dynamic_index_in_dim(snapshots[SWEEPS - 1], my_band, 0, keepdims=False)
    zp_tile = lax.dynamic_slice_in_dim(final, my_tile * tile_rows, tile_rows, axis=0)
    my_row = (my_tile * blocks + my_band * mine) // pack
    zp_two = lax.dynamic_slice_in_dim(snapshots, my_row, 1, axis=2)
    star_means, partial = pl.pallas_call(
        functools.partial(finish_kernel, bands, obs, list_len, rows),
        out_shape=(
            jax.ShapeDtypeStruct((1, stars), jnp.float32),
            jax.ShapeDtypeStruct((8, LANES), jnp.float32),
        ),
        in_specs=[smem, vmem, vmem, vmem, vmem],
        out_specs=(vmem, vmem),
        name="finish",
    )(mixing, data, own, zp_two, zp_tile)
    slab = (8, LANES)
    total = pl.pallas_call(
        functools.partial(total_kernel, tiles, bands),
        out_shape=jax.ShapeDtypeStruct(slab, jnp.float32),
        in_specs=[vmem],
        out_specs=vmem,
        scratch_shapes=[
            pltpu.VMEM((bands,) + slab, jnp.float32),
            pltpu.VMEM(slab, jnp.float32),
            pltpu.VMEM((tiles,) + slab, jnp.float32),
            pltpu.SemaphoreType.DMA((peers,)),
            pltpu.SemaphoreType.DMA((peers,)),
        ],
        compiler_params=pltpu.CompilerParams(collective_id=1, has_side_effects=True),
        name="total",
    )(partial)
    misfit = total[0, : SWEEPS * bands].reshape(SWEEPS, bands) / (obs * stars * tiles)
    misfit = lax.dynamic_slice_in_dim(misfit, my_band, 1, axis=1)

    tile_ids = jnp.mod(my_tile + jnp.arange(3, dtype=jnp.int32) - 1, tiles)

    def close(table):
        by_tile = table.reshape(tiles, tile_rows * LANES)
        parts = [lax.dynamic_index_in_dim(by_tile, tile_ids[n], 0, keepdims=False) for n in range(3)]
        return jnp.concatenate(parts)

    close_fields = close(all_fields)
    is_mine = (owner == my_tile)[:, None]
    rank = jnp.sum((is_mine & (field_no < close_fields[None])).astype(jnp.int32), axis=0)
    has = jnp.sum((is_mine & (field_no == close_fields[None])).astype(jnp.int32), axis=0) > 0
    rank = jnp.where(has, rank, owned)
    entry_no = jnp.arange(close_fields.shape[0], dtype=jnp.int32)[:, None]
    hit = rank[:, None] == jnp.arange(owned, dtype=jnp.int32)[None]
    chosen = jnp.max(jnp.where(hit, entry_no, -1), axis=0)
    own_zp = jnp.sum(jnp.where(chosen[None] == entry_no, close(final)[:, None], 0.0), axis=0)
    return own_zp[None], star_means, misfit


def solution(mesh):
    in_specs = (
        P("band", None, "sky"),
        P("band", None, "sky"),
        P("band", None, "sky"),
        P("sky", None),
        P(),
        P(),
        P(),
    )
    out_specs = (P("band", "sky"), P("band", "sky"), P(None, "band"))
    return jax.shard_map(body, mesh=mesh, in_specs=in_specs, out_specs=out_specs, check_vma=False)
```
